256 devices in a mesh: gx: 16 (over z, core), gy: 16 (over y, x).
Axes of the slice: x: 4, y: 4, z: 8, core: 2. Of those that a mesh axis runs over, the one named last changes fastest.
Arguments:
- bottom_in: bfloat16 [65536, 256], P(('gx', 'gy')), may hold values from -6 to 6
- bottom_pre: bfloat16 [65536, 128], P(('gx', 'gy')), may hold values from -6 to 6
- pooled: bfloat16 [65536, 2, 128], P(('gx', 'gy')), may hold values from -6 to 6
- top_pre: bfloat16 [65536, 1024], P(('gx', 'gy')), may hold values from -6 to 6
- top_cotangent: bfloat16 [65536, 1024], P(('gx', 'gy')), may hold values from -0.75 to 0.75
- top_weight: bfloat16 [384, 1024], replicated, may hold values from -0.5 to 0.5
- lookup_owner: int32 [65536, 2, 32], P(('gx', 'gy')), may hold values from 0 to 255, as said below
- lookup_row: int32 [65536, 2, 32], P(('gx', 'gy')), may hold values from 0 to 2047
Outputs:
- table_grad: float32 [2, 524288, 128], P(None, ('gx', 'gy'))
- top_weight_grad: float32 [384, 1024], P('gy')
- top_bias_grad: float32 [1024], P('gy')
- bottom_weight_grad: float32 [256, 128], P('gy')
The draws below stay inside these ranges and needn't reach their ends.
Inputs may be any that keep to these rules, and one draw needn't show every extreme that they name: `lookup_owner`: row r of a table with r = owner * 2048 + row is held by device owner in the order of gx+gy. Among the lookups of one device's 256 bags and one table, every owner number appears at most 64 times, and one owner number, the same for all devices of that table, exactly 64 times.
All inputs are finite; a program needn't handle non-finite values.
Results may differ from the reference program's by a relative error of at most 0.003.
Values may be sent and summed in bfloat16 or wider, within the bound.
No kernel may reach another device: no remote copies, remote signals or barrier semaphores. Data moves between devices by JAX's collectives and lax.ppermute only.
A program may use at most 128 MiB of HBM per device.

```python
import math
import jax
import jax.numpy as jnp
import numpy as np
from jax import lax

D = 128
TOP = 1024
BOT_IN = 256
TABLES = 2
BAG = 32
ROWS_DEV = 2048
B_DEV = 256
BATCH = 65536
ROWS = 524288
TOP_IN = 384
CAP = 64
DEVICES = 256


def draw_lookup_owner(key, part):
    hot_key = jax.random.fold_in(key, 11)
    mix_key = jax.random.fold_in(key, 23)
    hot_owner = jax.random.randint(hot_key, (TABLES,), 0, DEVICES)
    spread = B_DEV * BAG - CAP
    others_base = jnp.repeat(jnp.arange(1, DEVICES, dtype=jnp.int32), CAP)

    def one_list(inner_key, hot_value):
        first_key = jax.random.fold_in(inner_key, 1)
        second_key = jax.random.fold_in(inner_key, 2)
        chosen = jax.random.permutation(first_key, others_base)[:spread]
        listed = jnp.concatenate([jnp.zeros((CAP,), jnp.int32), chosen.astype(jnp.int32)])
        listed = jax.random.permutation(second_key, listed)
        return (listed + hot_value) % DEVICES
    list_keys = jax.random.split(mix_key, DEVICES * TABLES)
    hot_all = jnp.tile(hot_owner, DEVICES)
    drawn = jax.vmap(one_list)(list_keys, hot_all)
    drawn = drawn.reshape(DEVICES, TABLES, B_DEV, BAG).transpose(0, 2, 1, 3)
    return drawn.reshape(DEVICES * B_DEV, TABLES, BAG).astype(jnp.int32)


def set_ends(values, key, low, top_value):
    extent = values.shape
    place = [jax.random.randint(jax.random.fold_in(key, axis), (), 0, extent[axis]) for axis in range(len(extent))]
    values = values.at[tuple(place)].set(low)
    longest = extent.index(max(extent))
    place[longest] = (place[longest] + 1) % extent[longest]
    return values.at[tuple(place)].set(top_value)


def raised(result, own_key, source, target, parts, factor):
    owner, partner = [(jnp.arange(result.shape[axis_at]) // (result.shape[axis_at] // parts)).reshape([-1 if axis == axis_at else 1 for axis in range(result.ndim)]) for axis_at in (source, target)]
    chosen = jax.random.permutation(own_key, parts)[partner]
    strong = (owner == chosen) | (owner == (partner + parts // 2) % parts)
    return jnp.where(strong, factor * result, result)


def block_levels(stream_key, dims, shards, smallest, top_value):
    def one(dim, shards_of):
        heights = jax.random.uniform(jax.random.fold_in(jax.random.fold_in(stream_key, 6), dim), (shards_of,), jnp.float32, smallest / len(shards), top_value / len(shards))
        return jnp.repeat(jnp.exp(heights), dims[dim] // shards_of).reshape((-1,) + (1,) * (len(dims) - dim - 1))

    gain = one(*shards[0])
    for cut in shards[1:]:
        gain = gain * one(*cut)
    return gain


def rank_bounds(number_of, slope):
    loads = [(1 << 20) // math.isqrt(standing ** slope) + 1 for standing in range(1, number_of + 1)]
    width = 1 + sum(loads) // (1 << 30)
    return np.cumsum(np.array([max(1, weight // width) for weight in loads]))


def ranked(own_key, extent, amount, skew):
    listing = rank_bounds(amount, skew)
    ticket = jax.random.randint(jax.random.fold_in(own_key, 1), extent, 0, int(listing[amount - 1]))
    standing = jnp.searchsorted(jnp.asarray(listing, jnp.int32), ticket, side="right")
    return jax.random.permutation(jax.random.fold_in(own_key, 2), amount)[standing].astype(jnp.int32)


def noise(key, shape, scale, reach, shards=(), kind=jnp.bfloat16):
    gain = block_levels(key, shape, shards, -0.22, 0.18) if shards else 1.0
    values = jax.random.normal(key, shape, jnp.float32) * scale * gain
    return jnp.minimum(jnp.maximum(values, -reach), reach).astype(kind)


def bell_draw_with(rng, extent, deviation, reach, pieces, heavy, held_as=jnp.bfloat16):
    values = deviation * jax.random.normal(rng, extent, jnp.float32)
    if pieces:
        values = values * block_levels(rng, extent, pieces, -0.22, 0.18)
    return jnp.clip(raised(values, jax.random.fold_in(rng, 3), *heavy), -reach, reach).astype(held_as)


def setup_inputs(seed: int = 0) -> dict:
    splits = jax.random.split(jax.random.key(seed), 9)
    return {
        "bottom_in": noise(splits[0], (BATCH, BOT_IN), 1.0, 6.0, ((0, 256),)),
        "bottom_pre": noise(splits[1], (BATCH, D), 1.0, 6.0, ((0, 256),)),
        "pooled": noise(splits[2], (BATCH, TABLES, D), 1.0, 6.0, ((0, 256),)),
        "top_pre": noise(splits[3], (BATCH, TOP), 1.0, 6.0, ((0, 256),)),
        "top_cotangent": bell_draw_with(splits[4], (BATCH, TOP), TOP ** -0.5, 0.75, ((0, 256),), (0, 1, 256, 6.0)),
        "top_weight": noise(splits[5], (TOP_IN, TOP), D ** -0.5, 0.5),
        "lookup_owner": draw_lookup_owner(jax.random.fold_in(splits[8], 71), 0),
        "lookup_row": set_ends(ranked(splits[7], (BATCH, TABLES, BAG), ROWS_DEV, 2), jax.random.fold_in(splits[7], 3), 0, ROWS_DEV - 1).astype(jnp.int32),
    }


def table_gradient(bag_grad, lookup_owner, lookup_row):
    slot_total = TABLES * ROWS
    accum = jnp.zeros((slot_total, D), jnp.float32)
    table_ids = jnp.arange(TABLES, dtype=jnp.int32)[None, :, None]

    def add_block(block, accum):
        start = (block * B_DEV).astype(jnp.int32)
        grads = lax.dynamic_slice_in_dim(bag_grad, start, B_DEV, 0)
        owners = lax.dynamic_slice_in_dim(lookup_owner, start, B_DEV, 0)
        rows_here = lax.dynamic_slice_in_dim(lookup_row, start, B_DEV, 0)
        target = table_ids * ROWS + owners * ROWS_DEV + rows_here
        values = jnp.broadcast_to(grads[:, :, None, :], (B_DEV, TABLES, BAG, D)).astype(jnp.float32)
        return accum.at[target.reshape(-1)].add(values.reshape(-1, D))

    accum = lax.fori_loop(0, BATCH // B_DEV, add_block, accum)
    return accum.reshape(TABLES, ROWS, D)


def reference(bottom_in, bottom_pre, pooled, top_pre, top_cotangent, top_weight, lookup_owner, lookup_row):
    top_grad = jnp.where(top_pre > 0, top_cotangent, jnp.zeros_like(top_cotangent))
    bottom_out = jnp.maximum(bottom_pre, jnp.zeros_like(bottom_pre))
    feature = jnp.concatenate([bottom_out, pooled.reshape(BATCH, TABLES * D)], axis=1)
    top_weight_grad = lax.dot_general(feature, top_grad, (((0,), (0,)), ((), ())), preferred_element_type=jnp.float32)
    top_bias_grad = jnp.sum(top_grad.astype(jnp.float32), axis=0)
    feature_grad = lax.dot_general(top_grad, top_weight, (((1,), (1,)), ((), ())), preferred_element_type=jnp.float32).astype(jnp.bfloat16)
    bottom_grad = jnp.where(bottom_pre > 0, feature_grad[:, :D], jnp.zeros_like(bottom_pre))
    bottom_weight_grad = lax.dot_general(bottom_in, bottom_grad, (((0,), (0,)), ((), ())), preferred_element_type=jnp.float32)
    bag_grad = feature_grad[:, D:].reshape(BATCH, TABLES, D)
    table_grad = table_gradient(bag_grad, lookup_owner, lookup_row)
    return table_grad, top_weight_grad, top_bias_grad, bottom_weight_grad
```

```python
import functools

import jax
import jax.numpy as jnp
from jax import lax
from jax.experimental import pallas as pl
from jax.experimental.pallas import tpu as pltpu
from jax.sharding import PartitionSpec as P


ROWS_DEV = 2048
CAP = 64
CORES = 2
SIDE = 4
GROUP = 8
PEERS = 2
FREE = 256
BAG_STEP = 4096
NT = (((1,), (1,)), ((), ()))
NN = (((1,), (0,)), ((), ()))


def exchange(x, axis):
    return lax.all_to_all(x, axis, split_axis=0, concat_axis=0, tiled=True)


def slot_kernel(owner_ref, row_ref, code_ref, member, column):
    tables, lookups, bags = owner_ref.shape
    owners = code_ref.shape[0]
    owner_ids = lax.broadcasted_iota(jnp.int32, (owners, bags), 0)
    slot_ids = lax.broadcasted_iota(jnp.int32, (CAP, bags), 0)
    bag_ids = lax.broadcasted_iota(jnp.int32, (CAP, bags), 1).astype(jnp.float32)
    earlier = (
        lax.broadcasted_iota(jnp.int32, (bags, bags), 0)
        < lax.broadcasted_iota(jnp.int32, (bags, bags), 1)
    ).astype(jnp.bfloat16)
    for t in range(tables):
        counts = jnp.zeros((owners, bags), jnp.float32)
        for j in range(lookups):
            hit = owner_ref[t, j : j + 1, :] == owner_ids
            counts = counts + jnp.where(hit, 1.0, 0.0)
        taken = lax.dot_general(
            counts.astype(jnp.bfloat16), earlier, NN, preferred_element_type=jnp.float32
        )
        for j in range(lookups):
            span = slice(j * bags, (j + 1) * bags)
            hit = owner_ref[t, j : j + 1, :] == owner_ids
            rank = jnp.sum(jnp.where(hit, taken, 0.0), axis=0, keepdims=True)
            one = jnp.where(hit, 1.0, 0.0)
            taken = taken + one
            member[:, span] = one.astype(jnp.bfloat16)
            place = rank.astype(jnp.int32) == slot_ids
            row = row_ref[t, j : j + 1, :] + FREE
            high = (row >> 8).astype(jnp.float32)
            low = (row & 255).astype(jnp.float32)
            column[0:CAP, span] = jnp.where(place, bag_ids, 0.0).astype(jnp.bfloat16)
            column[CAP : 2 * CAP, span] = jnp.where(place, high, 0.0).astype(jnp.bfloat16)
            column[2 * CAP : 3 * CAP, span] = jnp.where(place, low, 0.0).astype(jnp.bfloat16)
        found = lax.dot_general(member[...], column[...], NT, preferred_element_type=jnp.float32)
        code = (
            found[:, 0:CAP] * float(BAG_STEP)
            + found[:, CAP : 2 * CAP] * 256.0
            + found[:, 2 * CAP : 3 * CAP]
        )
        code_ref[:, t * CAP : (t + 1) * CAP] = code.astype(jnp.int32)


def slot_codes(owner_lists, row_lists, owners):
    tables, lookups, bags = owner_lists.shape
    return pl.pallas_call(
        slot_kernel,
        out_shape=jax.ShapeDtypeStruct((owners, tables * CAP), jnp.int32),
        scratch_shapes=[
            pltpu.VMEM((owners, lookups * bags), jnp.bfloat16),
            pltpu.VMEM((3 * CAP, lookups * bags), jnp.bfloat16),
        ],
        cost_estimate=pl.CostEstimate(
            flops=4 * 10**9, bytes_accessed=262144, transcendentals=0
        ),
        name="slots",
    )(owner_lists, row_lists)


def tall(row, height):
    return jnp.tile(jnp.broadcast_to(row, (16, row.shape[1])).astype(jnp.bfloat16), (height // 16, 1))


def paired(mine, other, lane, t):
    if t == 0:
        return jnp.where(lane < CAP, mine, pltpu.roll(other, CAP, 1))
    return jnp.where(lane < CAP, pltpu.roll(mine, CAP, 1), other)


def gather_kernel(_, mine_ref, other_ref, mine_grad, other_grad, out_ref):
    tables, width, bags = mine_grad.shape[1:]
    peers, lanes = mine_ref.shape[1:]
    mine, other = mine_ref[0], other_ref[0]
    lane = lax.broadcasted_iota(jnp.int32, (peers, lanes), 1)
    group = GROUP * lanes
    bag_ids = lax.broadcasted_iota(jnp.int32, (bags, group), 0).astype(jnp.float32)
    bag_ids = bag_ids.astype(jnp.bfloat16)
    one = jnp.ones((), jnp.bfloat16)
    zero = jnp.zeros((), jnp.bfloat16)
    first = (lax.broadcasted_iota(jnp.int32, (width, group), 1) & (lanes - 1)) < CAP
    line = lax.broadcasted_iota(jnp.int32, (16, lanes), 0)
    keys = [jnp.zeros((16, lanes), jnp.float32) for _ in range(peers)]
    for t in range(tables):
        code = paired(mine, other, lane, t)
        bag = (code >> 12).astype(jnp.float32)
        row = code & (BAG_STEP - 1)
        high = (row >> 8).astype(jnp.float32)
        low = (row & 255).astype(jnp.float32)
        both = jnp.concatenate([mine_grad[0, t], other_grad[0, t]], axis=0)
        span = slice(t * width, (t + 1) * width)
        for y in range(0, peers, GROUP):
            wanted = jnp.concatenate([bag[y + u : y + u + 1] for u in range(GROUP)], axis=1)
            pick = jnp.where(bag_ids == tall(wanted, bags), one, zero)
            got = lax.dot_general(both, pick, NN, preferred_element_type=jnp.float32)
            value = jnp.where(first, got[:width], got[width:]).astype(jnp.bfloat16)
            for u in range(GROUP):
                out_ref[y + u, span, :] = value[:, u * lanes : (u + 1) * lanes]
        for y in range(peers):
            keys[y] = jnp.where(line == 2 * t, high[y : y + 1], keys[y])
            keys[y] = jnp.where(line == 2 * t + 1, low[y : y + 1], keys[y])
    for y in range(peers):
        out_ref[y, tables * width :, :] = keys[y].astype(jnp.bfloat16)


def gathered(order, codes, mine, other):
    steps, tables, width, bags = mine.shape
    peers, lanes = codes.shape[1:]
    rows = tables * width + 16
    return pl.pallas_call(
        gather_kernel,
        grid_spec=pltpu.PrefetchScalarGridSpec(
            num_scalar_prefetch=1,
            grid=(steps,),
            in_specs=[
                pl.BlockSpec((1, peers, lanes), lambda i, order: (order[0, i], 0, 0)),
                pl.BlockSpec((1, peers, lanes), lambda i, order: (order[1, i], 0, 0)),
                pl.BlockSpec((1, tables, width, bags), lambda i, order: (i, 0, 0, 0)),
                pl.BlockSpec((1, tables, width, bags), lambda i, order: (i, 0, 0, 0)),
            ],
            out_specs=pl.BlockSpec((peers, rows, lanes), lambda i, order: (0, 0, i)),
        ),
        out_shape=jax.ShapeDtypeStruct((peers, rows, 2 * steps * CAP), jnp.bfloat16),
        cost_estimate=pl.CostEstimate(
            flops=8 * 10**9, bytes_accessed=12 * 2**20, transcendentals=0
        ),
        name="gather",
    )(order, codes, codes, mine, other)


def scatter_kernel(t, *refs):
    value_ref, key_ref, out_ref, total = refs[0], refs[1], refs[-2], refs[-1]
    peers, width, slots = value_ref.shape
    quarter = 256
    half = ROWS_DEV // 2
    step = pl.program_id(0)

    @pl.when(step == 0)
    def _():
        total[...] = jnp.zeros_like(total)

    row_ids = lax.broadcasted_iota(jnp.int32, (quarter, slots), 0).astype(jnp.float32)
    row_ids = row_ids.astype(jnp.bfloat16)
    one = jnp.ones((), jnp.bfloat16)
    zero = jnp.zeros((), jnp.bfloat16)
    hits, spreads = [], []
    for p in range(peers):
        keys = key_ref[p].astype(jnp.float32)
        high = keys[2 * t : 2 * t + 1] - 1.0
        low = keys[2 * t + 1 : 2 * t + 2]
        lower = tall(jnp.where(high < 4.0, 1.0, 0.0), width)
        upper = tall(jnp.where(high < 4.0, 0.0, 1.0), width)
        value = value_ref[p]
        spreads.append(jnp.concatenate([value * lower, value * upper], axis=0))
        parts = []
        for k in range(half // quarter):
            here = (high == float(k)) | (high == float(k + 4))
            key = tall(jnp.where(here, low, -1.0), quarter)
            parts.append(jnp.where(row_ids == key, one, zero))
        hits.append(jnp.concatenate(parts, axis=0))
    total[...] += lax.dot_general(
        jnp.concatenate(hits, axis=1),
        jnp.concatenate(spreads, axis=1),
        NT,
        preferred_element_type=jnp.float32,
    )

    @pl.when(step == pl.num_programs(0) - 1)
    def _():
        out_ref[0, :half, :] = total[:, :width]
        out_ref[0, half:, :] = total[:, width:]


def scattered(t, tables, values, width, before):
    peers, _, slots = values.shape
    in_specs = [
        pl.BlockSpec((PEERS, width, slots), lambda i: (i, t, 0)),
        pl.BlockSpec((PEERS, 16, slots), lambda i: (i, tables * width // 16, 0)),
    ]
    args = [values, values]
    aliases = {}
    if before is not None:
        in_specs.append(pl.BlockSpec(memory_space=pl.ANY))
        args.append(before)
        aliases = {2: 0}
    return pl.pallas_call(
        functools.partial(scatter_kernel, t),
        grid=(peers // PEERS,),
        in_specs=in_specs,
        out_specs=pl.BlockSpec((1, ROWS_DEV, width), lambda i: (t, 0, 0)),
        out_shape=jax.ShapeDtypeStruct((tables, ROWS_DEV, width), jnp.float32),
        scratch_shapes=[pltpu.VMEM((ROWS_DEV // 2, 2 * width), jnp.float32)],
        input_output_aliases=aliases,
        cost_estimate=pl.CostEstimate(
            flops=2 * 10**10, bytes_accessed=6 * 2**20, transcendentals=0
        ),
        name="scatter",
    )(*args)


def passed(part, place, dim, target, devices):
    peers = part.shape[dim]
    total = lax.dynamic_index_in_dim(part, place, dim, keepdims=False)
    for k in range(1, peers):
        give = lax.dynamic_index_in_dim(part, (place + k) % peers, dim, keepdims=False)
        total = total + lax.ppermute(give, "gy", [(i, target(i, k)) for i in range(devices)])
    return total


def body(
    bottom_in, bottom_pre, pooled, top_pre, top_cotangent, top_weight, lookup_owner, lookup_row
):
    bags, tables, width = pooled.shape
    gx = lax.axis_size("gx")
    gy = lax.axis_size("gy")
    f32 = jnp.float32
    bf16 = jnp.bfloat16
    me = lax.axis_index("gx")
    chips = gx // CORES
    columns = [[z * CORES + c for z in range(chips)] for c in range(CORES)]

    owner_lists = lookup_owner.transpose(1, 2, 0)
    row_lists = lookup_row.transpose(1, 2, 0)
    codes = slot_codes(owner_lists, row_lists, gx * gy)
    codes = exchange(codes.reshape(gx, gy, tables * CAP), "gx")
    chip = jnp.arange(chips, dtype=jnp.int32)
    order = jnp.stack(
        [chip * CORES + (me & 1), chip * CORES + (1 - (me & 1))]
    ).astype(jnp.int32)

    top_grad = jnp.where(top_pre > 0, top_cotangent, jnp.zeros_like(top_cotangent))
    grad = lax.dot_general(top_weight[width:], top_grad, NT, preferred_element_type=f32)
    grad = grad.astype(bf16).reshape(tables, width, bags)
    copies = jnp.broadcast_to(grad, (chips, tables, width, bags))
    mine = lax.all_to_all(
        copies, "gx", split_axis=0, concat_axis=0, axis_index_groups=columns, tiled=True
    )
    other = lax.ppermute(mine, "gx", [(i, i ^ 1) for i in range(gx)])
    payload = gathered(order, codes, mine, other)

    bottom_out = jnp.maximum(bottom_pre, jnp.zeros_like(bottom_pre))
    feature = jnp.concatenate([bottom_out, pooled.reshape(bags, tables * width)], axis=1)
    first = lax.dot_general(top_grad, top_weight[:width], NT, preferred_element_type=f32)
    bottom_grad = jnp.where(bottom_pre > 0, first.astype(bf16), jnp.zeros_like(bottom_pre))
    top_part = lax.dot_general(
        feature, top_grad, (((0,), (0,)), ((), ())), preferred_element_type=f32
    )
    bias_part = jnp.sum(top_grad.astype(f32), axis=0)
    bottom_part = lax.dot_general(
        bottom_in, bottom_grad, (((0,), (0,)), ((), ())), preferred_element_type=f32
    )
    top_in, top = top_part.shape
    bottom_width = bottom_part.shape[0]
    top_rows = top_in // gy
    bottom_rows = bottom_width // gy * width // top
    tail = jnp.concatenate(
        [
            bottom_part.reshape(gy, bottom_rows, top),
            jnp.pad(bias_part.reshape(gy, 1, top // gy), ((0, 0), (0, 0), (0, top - top // gy))),
        ],
        axis=1,
    )
    tail = jnp.pad(tail, ((0, 0), (0, 8 - tail.shape[1]), (0, 0)))
    part = jnp.concatenate([top_part.reshape(gy, top_rows, top), tail], axis=1)
    half = part.shape[1] // CORES
    keep = lax.dynamic_slice_in_dim(part, (me & 1) * half, half, 1)
    give = lax.dynamic_slice_in_dim(part, (1 - (me & 1)) * half, half, 1)
    part = keep + lax.ppermute(give, "gx", [(i, i ^ 1) for i in range(gx)])
    part = part.reshape(gy // SIDE, SIDE, half, top)
    place = lax.axis_index("gy")
    part = passed(part, place % SIDE, 1, lambda i, k: i // SIDE * SIDE + (i + k) % SIDE, gy)
    part = passed(part, place // SIDE, 0, lambda i, k: (i + k * SIDE) % gy, gy)
    payload, part = lax.optimization_barrier((payload, part))
    arrived = exchange(payload, "gy")
    part, arrived = lax.optimization_barrier((part, arrived))

    part = lax.all_to_all(
        part.reshape(chips, half // chips, top),
        "gx", split_axis=0, concat_axis=0, axis_index_groups=columns, tiled=True,
    )
    part = jnp.sum(part, axis=0)
    total = exchange(jnp.broadcast_to(part, (gx, *part.shape)), "gx")
    total = total.reshape(chips, CORES, *part.shape).transpose(1, 0, 2, 3).reshape(-1, top)
    top_weight_grad = total[:top_rows]
    bottom_weight_grad = total[top_rows : top_rows + bottom_rows].reshape(-1, width)
    top_bias_grad = total[top_rows + bottom_rows, : top // gy]

    table_grad = None
    for t in range(tables):
        table_grad = scattered(t, tables, arrived, width, table_grad)
    return (table_grad, top_weight_grad, top_bias_grad, bottom_weight_grad)


def solution(mesh):
    return jax.shard_map(
        body,
        mesh=mesh,
        in_specs=(
            P(("gx", "gy"), None),
            P(("gx", "gy"), None),
            P(("gx", "gy"), None, None),
            P(("gx", "gy"), None),
            P(("gx", "gy"), None),
            P(),
            P(("gx", "gy"), None, None),
            P(("gx", "gy"), None, None),
        ),
        out_specs=(P(None, ("gx", "gy"), None), P("gy", None), P("gy"), P("gy", None)),
        check_vma=False,
    )
```

```python
import functools

import jax
import jax.numpy as jnp
from jax import lax
from jax.experimental import pallas as pl
from jax.experimental.pallas import tpu as pltpu
from jax.sharding import PartitionSpec as P


ROWS_DEV = 2048
CAP = 64
CORES = 2
SIDE = 4
GROUP = 8
PEERS = 4
FREE = 256
BAG_STEP = 4096
NT = (((1,), (1,)), ((), ()))
NN = (((1,), (0,)), ((), ()))


def exchange(x, axis):
    return lax.all_to_all(x, axis, split_axis=0, concat_axis=0, tiled=True)


def slot_kernel(owner_ref, row_ref, code_ref, member, column):
    tables, lookups, bags = owner_ref.shape
    owners = code_ref.shape[0]
    owner_ids = lax.broadcasted_iota(jnp.int32, (owners, bags), 0)
    slot_ids = lax.broadcasted_iota(jnp.int32, (CAP, bags), 0)
    bag_ids = lax.broadcasted_iota(jnp.int32, (CAP, bags), 1).astype(jnp.float32)
    earlier = (
        lax.broadcasted_iota(jnp.int32, (bags, bags), 0)
        < lax.broadcasted_iota(jnp.int32, (bags, bags), 1)
    ).astype(jnp.bfloat16)
    for t in range(tables):
        counts = jnp.zeros((owners, bags), jnp.float32)
        for j in range(lookups):
            hit = owner_ref[t, j : j + 1, :] == owner_ids
            counts = counts + jnp.where(hit, 1.0, 0.0)
        taken = lax.dot_general(
            counts.astype(jnp.bfloat16), earlier, NN, preferred_element_type=jnp.float32
        )
        for j in range(lookups):
            span = slice(j * bags, (j + 1) * bags)
            hit = owner_ref[t, j : j + 1, :] == owner_ids
            rank = jnp.sum(jnp.where(hit, taken, 0.0), axis=0, keepdims=True)
            one = jnp.where(hit, 1.0, 0.0)
            taken = taken + one
            member[:, span] = one.astype(jnp.bfloat16)
            place = rank.astype(jnp.int32) == slot_ids
            row = row_ref[t, j : j + 1, :] + FREE
            high = (row >> 8).astype(jnp.float32)
            low = (row & 255).astype(jnp.float32)
            column[0:CAP, span] = jnp.where(place, bag_ids, 0.0).astype(jnp.bfloat16)
            column[CAP : 2 * CAP, span] = jnp.where(place, high, 0.0).astype(jnp.bfloat16)
            column[2 * CAP : 3 * CAP, span] = jnp.where(place, low, 0.0).astype(jnp.bfloat16)
        found = lax.dot_general(member[...], column[...], NT, preferred_element_type=jnp.float32)
        code = (
            found[:, 0:CAP] * float(BAG_STEP)
            + found[:, CAP : 2 * CAP] * 256.0
            + found[:, 2 * CAP : 3 * CAP]
        )
        code_ref[:, t * CAP : (t + 1) * CAP] = code.astype(jnp.int32)


def slot_codes(owner_lists, row_lists, owners):
    tables, lookups, bags = owner_lists.shape
    return pl.pallas_call(
        slot_kernel,
        out_shape=jax.ShapeDtypeStruct((owners, tables * CAP), jnp.int32),
        scratch_shapes=[
            pltpu.VMEM((owners, lookups * bags), jnp.bfloat16),
            pltpu.VMEM((3 * CAP, lookups * bags), jnp.bfloat16),
        ],
        cost_estimate=pl.CostEstimate(
            flops=10**6, bytes_accessed=262144, transcendentals=0
        ),
        name="slots",
    )(owner_lists, row_lists)


def tall(row, height):
    return jnp.tile(jnp.broadcast_to(row, (16, row.shape[1])).astype(jnp.bfloat16), (height // 16, 1))


def paired(mine, other, lane, t):
    if t == 0:
        return jnp.where(lane < CAP, mine, pltpu.roll(other, CAP, 1))
    return jnp.where(lane < CAP, pltpu.roll(mine, CAP, 1), other)


def gather_kernel(_, mine_ref, other_ref, mine_grad, other_grad, out_ref):
    tables, width, bags = mine_grad.shape[1:]
    peers, lanes = mine_ref.shape[1:]
    mine, other = mine_ref[0], other_ref[0]
    lane = lax.broadcasted_iota(jnp.int32, (peers, lanes), 1)
    group = GROUP * lanes
    bag_ids = lax.broadcasted_iota(jnp.int32, (bags, group), 0).astype(jnp.float32)
    bag_ids = bag_ids.astype(jnp.bfloat16)
    one = jnp.ones((), jnp.bfloat16)
    zero = jnp.zeros((), jnp.bfloat16)
    first = (lax.broadcasted_iota(jnp.int32, (width, group), 1) & (lanes - 1)) < CAP
    line = lax.broadcasted_iota(jnp.int32, (16, lanes), 0)
    keys = [jnp.zeros((16, lanes), jnp.float32) for _ in range(peers)]
    for t in range(tables):
        code = paired(mine, other, lane, t)
        bag = (code >> 12).astype(jnp.float32)
        row = code & (BAG_STEP - 1)
        high = (row >> 8).astype(jnp.float32)
        low = (row & 255).astype(jnp.float32)
        both = jnp.concatenate([mine_grad[0, t], other_grad[0, t]], axis=0)
        span = slice(t * width, (t + 1) * width)
        for y in range(0, peers, GROUP):
            wanted = jnp.concatenate([bag[y + u : y + u + 1] for u in range(GROUP)], axis=1)
            pick = jnp.where(bag_ids == tall(wanted, bags), one, zero)
            got = lax.dot_general(both, pick, NN, preferred_element_type=jnp.float32)
            value = jnp.where(first, got[:width], got[width:]).astype(jnp.bfloat16)
            for u in range(GROUP):
                out_ref[y + u, span, :] = value[:, u * lanes : (u + 1) * lanes]
        for y in range(peers):
            keys[y] = jnp.where(line == 2 * t, high[y : y + 1], keys[y])
            keys[y] = jnp.where(line == 2 * t + 1, low[y : y + 1], keys[y])
    for y in range(peers):
        out_ref[y, tables * width :, :] = keys[y].astype(jnp.bfloat16)


def gathered(order, codes, mine, other):
    steps, tables, width, bags = mine.shape
    peers, lanes = codes.shape[1:]
    rows = tables * width + 16
    return pl.pallas_call(
        gather_kernel,
        grid_spec=pltpu.PrefetchScalarGridSpec(
            num_scalar_prefetch=1,
            grid=(steps,),
            in_specs=[
                pl.BlockSpec((1, peers, lanes), lambda i, order: (order[0, i], 0, 0)),
                pl.BlockSpec((1, peers, lanes), lambda i, order: (order[1, i], 0, 0)),
                pl.BlockSpec((1, tables, width, bags), lambda i, order: (i, 0, 0, 0)),
                pl.BlockSpec((1, tables, width, bags), lambda i, order: (i, 0, 0, 0)),
            ],
            out_specs=pl.BlockSpec((peers, rows, lanes), lambda i, order: (0, 0, i)),
        ),
        out_shape=jax.ShapeDtypeStruct((peers, rows, 2 * steps * CAP), jnp.bfloat16),
        cost_estimate=pl.CostEstimate(
            flops=8 * 10**9, bytes_accessed=12 * 2**20, transcendentals=0
        ),
        name="gather",
    )(order, codes, codes, mine, other)


def scatter_kernel(t, *refs):
    value_ref, key_ref, out_ref, total = refs[0], refs[1], refs[-2], refs[-1]
    peers, width, slots = value_ref.shape
    quarter = 256
    half = ROWS_DEV // 2
    step = pl.program_id(0)

    @pl.when(step == 0)
    def _():
        total[...] = jnp.zeros_like(total)

    row_ids = lax.broadcasted_iota(jnp.int32, (quarter, slots), 0).astype(jnp.float32)
    row_ids = row_ids.astype(jnp.bfloat16)
    one = jnp.ones((), jnp.bfloat16)
    zero = jnp.zeros((), jnp.bfloat16)
    hits, spreads = [], []
    for p in range(peers):
        keys = key_ref[p].astype(jnp.float32)
        high = keys[2 * t : 2 * t + 1] - 1.0
        low = keys[2 * t + 1 : 2 * t + 2]
        lower = tall(jnp.where(high < 4.0, 1.0, 0.0), width)
        upper = tall(jnp.where(high < 4.0, 0.0, 1.0), width)
        value = value_ref[p]
        spreads.append(jnp.concatenate([value * lower, value * upper], axis=0))
        parts = []
        for k in range(half // quarter):
            here = (high == float(k)) | (high == float(k + 4))
            key = tall(jnp.where(here, low, -1.0), quarter)
            parts.append(jnp.where(row_ids == key, one, zero))
        hits.append(jnp.concatenate(parts, axis=0))
    total[...] += lax.dot_general(
        jnp.concatenate(hits, axis=1),
        jnp.concatenate(spreads, axis=1),
        NT,
        preferred_element_type=jnp.float32,
    )

    @pl.when(step == pl.num_programs(0) - 1)
    def _():
        out_ref[0, :half, :] = total[:, :width]
        out_ref[0, half:, :] = total[:, width:]


def scattered(t, tables, values, width, before):
    peers, _, slots = values.shape
    in_specs = [
        pl.BlockSpec((PEERS, width, slots), lambda i: (i, t, 0)),
        pl.BlockSpec((PEERS, 16, slots), lambda i: (i, tables * width // 16, 0)),
    ]
    args = [values, values]
    aliases = {}
    if before is not None:
        in_specs.append(pl.BlockSpec(memory_space=pl.ANY))
        args.append(before)
        aliases = {2: 0}
    return pl.pallas_call(
        functools.partial(scatter_kernel, t),
        grid=(peers // PEERS,),
        in_specs=in_specs,
        out_specs=pl.BlockSpec((1, ROWS_DEV, width), lambda i: (t, 0, 0)),
        out_shape=jax.ShapeDtypeStruct((tables, ROWS_DEV, width), jnp.float32),
        scratch_shapes=[pltpu.VMEM((ROWS_DEV // 2, 2 * width), jnp.float32)],
        input_output_aliases=aliases,
        cost_estimate=pl.CostEstimate(
            flops=2 * 10**10, bytes_accessed=6 * 2**20, transcendentals=0
        ),
        name="scatter",
    )(*args)


def passed(part, place, dim, target, devices):
    peers = part.shape[dim]
    total = lax.dynamic_index_in_dim(part, place, dim, keepdims=False)
    for k in range(1, peers):
        give = lax.dynamic_index_in_dim(part, (place + k) % peers, dim, keepdims=False)
        total = total + lax.ppermute(give, "gy", [(i, target(i, k)) for i in range(devices)])
    return total


def body(
    bottom_in, bottom_pre, pooled, top_pre, top_cotangent, top_weight, lookup_owner, lookup_row
):
    bags, tables, width = pooled.shape
    gx = lax.axis_size("gx")
    gy = lax.axis_size("gy")
    f32 = jnp.float32
    bf16 = jnp.bfloat16
    me = lax.axis_index("gx")
    chips = gx // CORES
    columns = [[z * CORES + c for z in range(chips)] for c in range(CORES)]

    owner_lists = lookup_owner.transpose(1, 2, 0)
    row_lists = lookup_row.transpose(1, 2, 0)
    codes = slot_codes(owner_lists, row_lists, gx * gy)
    codes = exchange(codes.reshape(gx, gy, tables * CAP), "gx")
    chip = jnp.arange(chips, dtype=jnp.int32)
    order = jnp.stack(
        [chip * CORES + (me & 1), chip * CORES + (1 - (me & 1))]
    ).astype(jnp.int32)

    top_grad = jnp.where(top_pre > 0, top_cotangent, jnp.zeros_like(top_cotangent))
    grad = lax.dot_general(top_weight[width:], top_grad, NT, preferred_element_type=f32)
    grad = grad.astype(bf16).reshape(tables, width, bags)
    copies = jnp.broadcast_to(grad, (chips, tables, width, bags))
    top_grad, bottom_in, bottom_pre, pooled, copies = lax.optimization_barrier(
        (top_grad, bottom_in, bottom_pre, pooled, copies)
    )
    mine = lax.all_to_all(
        copies, "gx", split_axis=0, concat_axis=0, axis_index_groups=columns, tiled=True
    )
    bottom_out = jnp.maximum(bottom_pre, jnp.zeros_like(bottom_pre))
    feature = jnp.concatenate([bottom_out, pooled.reshape(bags, tables * width)], axis=1)
    first = lax.dot_general(top_grad, top_weight[:width], NT, preferred_element_type=f32)
    bottom_grad = jnp.where(bottom_pre > 0, first.astype(bf16), jnp.zeros_like(bottom_pre))
    top_part = lax.dot_general(
        feature, top_grad, (((0,), (0,)), ((), ())), preferred_element_type=f32
    )
    bias_part = jnp.sum(top_grad.astype(f32), axis=0)
    bottom_part = lax.dot_general(
        bottom_in, bottom_grad, (((0,), (0,)), ((), ())), preferred_element_type=f32
    )
    top_in, top = top_part.shape
    bottom_width = bottom_part.shape[0]
    top_rows = top_in // gy
    bottom_rows = bottom_width // gy * width // top
    tail = jnp.concatenate(
        [
            bottom_part.reshape(gy, bottom_rows, top),
            jnp.pad(bias_part.reshape(gy, 1, top // gy), ((0, 0), (0, 0), (0, top - top // gy))),
        ],
        axis=1,
    )
    tail = jnp.pad(tail, ((0, 0), (0, 8 - tail.shape[1]), (0, 0)))
    part = jnp.concatenate([top_part.reshape(gy, top_rows, top), tail], axis=1)
    half = part.shape[1] // CORES
    keep = lax.dynamic_slice_in_dim(part, (me & 1) * half, half, 1)
    give = lax.dynamic_slice_in_dim(part, (1 - (me & 1)) * half, half, 1)
    part = keep + lax.ppermute(give, "gx", [(i, i ^ 1) for i in range(gx)])
    part = part.reshape(gy // SIDE, SIDE, half, top)
    place = lax.axis_index("gy")
    part = passed(part, place % SIDE, 1, lambda i, k: i // SIDE * SIDE + (i + k) % SIDE, gy)
    mine, part = lax.optimization_barrier((mine, part))
    other = lax.ppermute(mine, "gx", [(i, i ^ 1) for i in range(gx)])
    payload = gathered(order, codes, mine, other)
    part = passed(part, place // SIDE, 0, lambda i, k: (i + k * SIDE) % gy, gy)
    payload, part = lax.optimization_barrier((payload, part))
    arrived = exchange(payload, "gy")
    part, arrived = lax.optimization_barrier((part, arrived))

    part = lax.all_to_all(
        part.reshape(chips, half // chips, top),
        "gx", split_axis=0, concat_axis=0, axis_index_groups=columns, tiled=True,
    )
    part = jnp.sum(part, axis=0)
    total = exchange(jnp.broadcast_to(part, (gx, *part.shape)), "gx")
    total = total.reshape(chips, CORES, *part.shape).transpose(1, 0, 2, 3).reshape(-1, top)
    top_weight_grad = total[:top_rows]
    bottom_weight_grad = total[top_rows : top_rows + bottom_rows].reshape(-1, width)
    top_bias_grad = total[top_rows + bottom_rows, : top // gy]

    table_grad = None
    for t in range(tables):
        table_grad = scattered(t, tables, arrived, width, table_grad)
    return (table_grad, top_weight_grad, top_bias_grad, bottom_weight_grad)


def solution(mesh):
    return jax.shard_map(
        body,
        mesh=mesh,
        in_specs=(
            P(("gx", "gy"), None),
            P(("gx", "gy"), None),
            P(("gx", "gy"), None, None),
            P(("gx", "gy"), None),
            P(("gx", "gy"), None),
            P(),
            P(("gx", "gy"), None, None),
            P(("gx", "gy"), None, None),
        ),
        out_specs=(P(None, ("gx", "gy"), None), P("gy", None), P("gy"), P("gy", None)),
        check_vma=False,
    )
```

```python
import functools

import jax
import jax.numpy as jnp
from jax import lax
from jax.experimental import pallas as pl
from jax.experimental.pallas import tpu as pltpu
from jax.sharding import PartitionSpec as P


ROWS_DEV = 2048
CAP = 64
CORES = 2
SIDE = 4
GROUP = 8
PEERS = 4
FREE = 256
BAG_STEP = 4096
NT = (((1,), (1,)), ((), ()))
NN = (((1,), (0,)), ((), ()))


def exchange(x, axis):
    return lax.all_to_all(x, axis, split_axis=0, concat_axis=0, tiled=True)


def slot_kernel(owner_ref, row_ref, code_ref, member, column):
    tables, lookups, bags = owner_ref.shape
    owners = code_ref.shape[0]
    owner_ids = lax.broadcasted_iota(jnp.int32, (owners, bags), 0)
    slot_ids = lax.broadcasted_iota(jnp.int32, (CAP, bags), 0)
    bag_ids = lax.broadcasted_iota(jnp.int32, (CAP, bags), 1).astype(jnp.float32)
    earlier = (
        lax.broadcasted_iota(jnp.int32, (bags, bags), 0)
        < lax.broadcasted_iota(jnp.int32, (bags, bags), 1)
    ).astype(jnp.bfloat16)
    for t in range(tables):
        counts = jnp.zeros((owners, bags), jnp.float32)
        for j in range(lookups):
            hit = owner_ref[t, j : j + 1, :] == owner_ids
            counts = counts + jnp.where(hit, 1.0, 0.0)
        taken = lax.dot_general(
            counts.astype(jnp.bfloat16), earlier, NN, preferred_element_type=jnp.float32
        )
        for j in range(lookups):
            span = slice(j * bags, (j + 1) * bags)
            hit = owner_ref[t, j : j + 1, :] == owner_ids
            rank = jnp.sum(jnp.where(hit, taken, 0.0), axis=0, keepdims=True)
            one = jnp.where(hit, 1.0, 0.0)
            taken = taken + one
            member[:, span] = one.astype(jnp.bfloat16)
            place = rank.astype(jnp.int32) == slot_ids
            row = row_ref[t, j : j + 1, :] + FREE
            high = (row >> 8).astype(jnp.float32)
            low = (row & 255).astype(jnp.float32)
            column[0:CAP, span] = jnp.where(place, bag_ids, 0.0).astype(jnp.bfloat16)
            column[CAP : 2 * CAP, span] = jnp.where(place, high, 0.0).astype(jnp.bfloat16)
            column[2 * CAP : 3 * CAP, span] = jnp.where(place, low, 0.0).astype(jnp.bfloat16)
        found = lax.dot_general(member[...], column[...], NT, preferred_element_type=jnp.float32)
        code = (
            found[:, 0:CAP] * float(BAG_STEP)
            + found[:, CAP : 2 * CAP] * 256.0
            + found[:, 2 * CAP : 3 * CAP]
        )
        code_ref[:, t * CAP : (t + 1) * CAP] = code.astype(jnp.int32)


def slot_codes(owner_lists, row_lists, owners):
    tables, lookups, bags = owner_lists.shape
    return pl.pallas_call(
        slot_kernel,
        out_shape=jax.ShapeDtypeStruct((owners, tables * CAP), jnp.int32),
        scratch_shapes=[
            pltpu.VMEM((owners, lookups * bags), jnp.bfloat16),
            pltpu.VMEM((3 * CAP, lookups * bags), jnp.bfloat16),
        ],
        cost_estimate=pl.CostEstimate(
            flops=10**6, bytes_accessed=262144, transcendentals=0
        ),
        name="slots",
    )(owner_lists, row_lists)


def tall(row, height):
    return jnp.tile(jnp.broadcast_to(row, (16, row.shape[1])).astype(jnp.bfloat16), (height // 16, 1))


def paired(mine, other, lane, t):
    if t == 0:
        return jnp.where(lane < CAP, mine, pltpu.roll(other, CAP, 1))
    return jnp.where(lane < CAP, pltpu.roll(mine, CAP, 1), other)


def gather_kernel(_, mine_ref, other_ref, mine_grad, other_grad, out_ref):
    tables, width, bags = mine_grad.shape[1:]
    peers, lanes = mine_ref.shape[1:]
    mine, other = mine_ref[0], other_ref[0]
    lane = lax.broadcasted_iota(jnp.int32, (peers, lanes), 1)
    group = GROUP * lanes
    bag_ids = lax.broadcasted_iota(jnp.int32, (bags, group), 0).astype(jnp.float32)
    bag_ids = bag_ids.astype(jnp.bfloat16)
    one = jnp.ones((), jnp.bfloat16)
    zero = jnp.zeros((), jnp.bfloat16)
    first = (lax.broadcasted_iota(jnp.int32, (width, group), 1) & (lanes - 1)) < CAP
    line = lax.broadcasted_iota(jnp.int32, (16, lanes), 0)
    keys = [jnp.zeros((16, lanes), jnp.float32) for _ in range(peers)]
    for t in range(tables):
        code = paired(mine, other, lane, t)
        bag = (code >> 12).astype(jnp.float32)
        row = code & (BAG_STEP - 1)
        high = (row >> 8).astype(jnp.float32)
        low = (row & 255).astype(jnp.float32)
        both = jnp.concatenate([mine_grad[0, t], other_grad[0, t]], axis=0)
        span = slice(t * width, (t + 1) * width)
        for y in range(0, peers, GROUP):
            wanted = jnp.concatenate([bag[y + u : y + u + 1] for u in range(GROUP)], axis=1)
            pick = jnp.where(bag_ids == tall(wanted, bags), one, zero)
            got = lax.dot_general(both, pick, NN, preferred_element_type=jnp.float32)
            value = jnp.where(first, got[:width], got[width:]).astype(jnp.bfloat16)
            for u in range(GROUP):
                out_ref[y + u, span, :] = value[:, u * lanes : (u + 1) * lanes]
        for y in range(peers):
            keys[y] = jnp.where(line == 2 * t, high[y : y + 1], keys[y])
            keys[y] = jnp.where(line == 2 * t + 1, low[y : y + 1], keys[y])
    for y in range(peers):
        out_ref[y, tables * width :, :] = keys[y].astype(jnp.bfloat16)


def gathered(order, codes, mine, other):
    steps, tables, width, bags = mine.shape
    peers, lanes = codes.shape[1:]
    rows = tables * width + 16
    return pl.pallas_call(
        gather_kernel,
        grid_spec=pltpu.PrefetchScalarGridSpec(
            num_scalar_prefetch=1,
            grid=(steps,),
            in_specs=[
                pl.BlockSpec((1, peers, lanes), lambda i, order: (order[0, i], 0, 0)),
                pl.BlockSpec((1, peers, lanes), lambda i, order: (order[1, i], 0, 0)),
                pl.BlockSpec((1, tables, width, bags), lambda i, order: (i, 0, 0, 0)),
                pl.BlockSpec((1, tables, width, bags), lambda i, order: (i, 0, 0, 0)),
            ],
            out_specs=pl.BlockSpec((peers, rows, lanes), lambda i, order: (0, 0, i)),
        ),
        out_shape=jax.ShapeDtypeStruct((peers, rows, 2 * steps * CAP), jnp.bfloat16),
        cost_estimate=pl.CostEstimate(
            flops=8 * 10**9, bytes_accessed=12 * 2**20, transcendentals=0
        ),
        name="gather",
    )(order, codes, codes, mine, other)


def scatter_kernel(t, *refs):
    value_ref, key_ref, out_ref, total = refs[0], refs[1], refs[-2], refs[-1]
    peers, width, slots = value_ref.shape
    quarter = 256
    half = ROWS_DEV // 2
    step = pl.program_id(0)

    @pl.when(step == 0)
    def _():
        total[...] = jnp.zeros_like(total)

    row_ids = lax.broadcasted_iota(jnp.int32, (quarter, slots), 0).astype(jnp.float32)
    row_ids = row_ids.astype(jnp.bfloat16)
    one = jnp.ones((), jnp.bfloat16)
    zero = jnp.zeros((), jnp.bfloat16)
    hits, spreads = [], []
    for p in range(peers):
        keys = key_ref[p].astype(jnp.float32)
        high = keys[2 * t : 2 * t + 1] - 1.0
        low = keys[2 * t + 1 : 2 * t + 2]
        lower = tall(jnp.where(high < 4.0, 1.0, 0.0), width)
        upper = tall(jnp.where(high < 4.0, 0.0, 1.0), width)
        value = value_ref[p]
        spreads.append(jnp.concatenate([value * lower, value * upper], axis=0))
        parts = []
        for k in range(half // quarter):
            here = (high == float(k)) | (high == float(k + 4))
            key = tall(jnp.where(here, low, -1.0), quarter)
            parts.append(jnp.where(row_ids == key, one, zero))
        hits.append(jnp.concatenate(parts, axis=0))
    total[...] += lax.dot_general(
        jnp.concatenate(hits, axis=1),
        jnp.concatenate(spreads, axis=1),
        NT,
        preferred_element_type=jnp.float32,
    )

    @pl.when(step == pl.num_programs(0) - 1)
    def _():
        out_ref[0, :half, :] = total[:, :width]
        out_ref[0, half:, :] = total[:, width:]


def scattered(t, tables, values, width, before):
    peers, _, slots = values.shape
    in_specs = [
        pl.BlockSpec((PEERS, width, slots), lambda i: (i, t, 0)),
        pl.BlockSpec((PEERS, 16, slots), lambda i: (i, tables * width // 16, 0)),
    ]
    args = [values, values]
    aliases = {}
    if before is not None:
        in_specs.append(pl.BlockSpec(memory_space=pl.ANY))
        args.append(before)
        aliases = {2: 0}
    return pl.pallas_call(
        functools.partial(scatter_kernel, t),
        grid=(peers // PEERS,),
        in_specs=in_specs,
        out_specs=pl.BlockSpec((1, ROWS_DEV, width), lambda i: (t, 0, 0)),
        out_shape=jax.ShapeDtypeStruct((tables, ROWS_DEV, width), jnp.float32),
        scratch_shapes=[pltpu.VMEM((ROWS_DEV // 2, 2 * width), jnp.float32)],
        input_output_aliases=aliases,
        cost_estimate=pl.CostEstimate(
            flops=2 * 10**10, bytes_accessed=6 * 2**20, transcendentals=0
        ),
        name="scatter",
    )(*args)


def passed(part, place, dim, target, devices):
    peers = part.shape[dim]
    total = lax.dynamic_index_in_dim(part, place, dim, keepdims=False)
    for k in range(1, peers):
        give = lax.dynamic_index_in_dim(part, (place + k) % peers, dim, keepdims=False)
        total = total + lax.ppermute(give, "gy", [(i, target(i, k)) for i in range(devices)])
    return total


def body(
    bottom_in, bottom_pre, pooled, top_pre, top_cotangent, top_weight, lookup_owner, lookup_row
):
    bags, tables, width = pooled.shape
    gx = lax.axis_size("gx")
    gy = lax.axis_size("gy")
    f32 = jnp.float32
    bf16 = jnp.bfloat16
    me = lax.axis_index("gx")
    chips = gx // CORES
    columns = [[z * CORES + c for z in range(chips)] for c in range(CORES)]

    owner_lists = lookup_owner.transpose(1, 2, 0)
    row_lists = lookup_row.transpose(1, 2, 0)
    codes = slot_codes(owner_lists, row_lists, gx * gy)
    codes = exchange(codes.reshape(gx, gy, tables * CAP), "gx")
    chip = jnp.arange(chips, dtype=jnp.int32)
    order = jnp.stack(
        [chip * CORES + (me & 1), chip * CORES + (1 - (me & 1))]
    ).astype(jnp.int32)

    top_grad = jnp.where(top_pre > 0, top_cotangent, jnp.zeros_like(top_cotangent))
    grad = lax.dot_general(top_weight[width:], top_grad, NT, preferred_element_type=f32)
    grad = grad.astype(bf16).reshape(tables, width, bags)
    copies = jnp.broadcast_to(grad, (chips, tables, width, bags))
    top_grad, bottom_in, bottom_pre, pooled, copies = lax.optimization_barrier(
        (top_grad, bottom_in, bottom_pre, pooled, copies)
    )
    mine = lax.all_to_all(
        copies, "gx", split_axis=0, concat_axis=0, axis_index_groups=columns, tiled=True
    )
    bottom_out = jnp.maximum(bottom_pre, jnp.zeros_like(bottom_pre))
    feature = jnp.concatenate([bottom_out, pooled.reshape(bags, tables * width)], axis=1)
    first = lax.dot_general(top_grad, top_weight[:width], NT, preferred_element_type=f32)
    bottom_grad = jnp.where(bottom_pre > 0, first.astype(bf16), jnp.zeros_like(bottom_pre))
    top_part = lax.dot_general(
        feature, top_grad, (((0,), (0,)), ((), ())), preferred_element_type=f32
    )
    bias_part = jnp.sum(top_grad.astype(f32), axis=0)
    bottom_part = lax.dot_general(
        bottom_in, bottom_grad, (((0,), (0,)), ((), ())), preferred_element_type=f32
    )
    top_in, top = top_part.shape
    bottom_width = bottom_part.shape[0]
    top_rows = top_in // gy
    bottom_rows = bottom_width // gy * width // top
    tail = jnp.concatenate(
        [
            bottom_part.reshape(gy, bottom_rows, top),
            jnp.pad(bias_part.reshape(gy, 1, top // gy), ((0, 0), (0, 0), (0, top - top // gy))),
        ],
        axis=1,
    )
    tail = jnp.pad(tail, ((0, 0), (0, 8 - tail.shape[1]), (0, 0)))
    part = jnp.concatenate([top_part.reshape(gy, top_rows, top), tail], axis=1)
    half = part.shape[1] // CORES
    keep = lax.dynamic_slice_in_dim(part, (me & 1) * half, half, 1)
    give = lax.dynamic_slice_in_dim(part, (1 - (me & 1)) * half, half, 1)
    part = keep + lax.ppermute(give, "gx", [(i, i ^ 1) for i in range(gx)])
    part = part.reshape(gy // SIDE, SIDE, half, top)
    place = lax.axis_index("gy")
    part = passed(part, place % SIDE, 1, lambda i, k: i // SIDE * SIDE + (i + k) % SIDE, gy)
    mine, part = lax.optimization_barrier((mine, part))
    other = lax.ppermute(mine, "gx", [(i, i ^ 1) for i in range(gx)])
    payload = gathered(order, codes, mine, other)
    part = passed(part, place // SIDE, 0, lambda i, k: (i + k * SIDE) % gy, gy)
    copies = jnp.broadcast_to(part, (chips, half, top))
    payload, copies = lax.optimization_barrier((payload, copies))
    arrived = exchange(payload, "gy")
    copies, arrived = lax.optimization_barrier((copies, arrived))
    part = lax.all_to_all(
        copies, "gx", split_axis=0, concat_axis=0, axis_index_groups=columns, tiled=True
    )
    part = jnp.sum(part, axis=0)
    twin = lax.ppermute(part, "gx", [(i, i ^ 1) for i in range(gx)])
    even = (me & 1) == 0
    total = jnp.concatenate([jnp.where(even, part, twin), jnp.where(even, twin, part)], axis=0)
    top_weight_grad = total[:top_rows]
    bottom_weight_grad = total[top_rows : top_rows + bottom_rows].reshape(-1, width)
    top_bias_grad = total[top_rows + bottom_rows, : top // gy]

    table_grad = None
    for t in range(tables):
        table_grad = scattered(t, tables, arrived, width, table_grad)
    return (table_grad, top_weight_grad, top_bias_grad, bottom_weight_grad)


def solution(mesh):
    return jax.shard_map(
        body,
        mesh=mesh,
        in_specs=(
            P(("gx", "gy"), None),
            P(("gx", "gy"), None),
            P(("gx", "gy"), None, None),
            P(("gx", "gy"), None),
            P(("gx", "gy"), None),
            P(),
            P(("gx", "gy"), None, None),
            P(("gx", "gy"), None, None),
        ),
        out_specs=(P(None, ("gx", "gy"), None), P("gy", None), P("gy"), P("gy", None)),
        check_vma=False,
    )
```
